512 devices in a mesh: paths: 16 (over y, core), contract: 32 (over z, x).
Axes of the slice: x: 4, y: 8, z: 8, core: 2. Of those that a mesh axis runs over, the one named last changes fastest.
Arguments:
- prices: float32 [1, 2048], P(None, 'paths'), may hold values from -6 to 6
- terminal: bfloat16 [2048, 2048, 128], P('contract', 'paths'), may hold values from -6 to 6
- band: int32 [2048], replicated, may hold values from 32 to 128
- position: int32 [2048], replicated, may hold values from 0 to 2047, as said below
- actions: int32 [2048, 3], replicated, may hold values from -3 to 3
- degree: int32 [2048], replicated, may hold values from 2 to 7
- volume: float32 [2048], replicated, may hold values from 0.05 to 0.5
Outputs:
- valued: bfloat16 [2048, 2048, 128], P('contract', 'paths')
The draws below stay inside these ranges and needn't reach their ends.
Inputs may be any that keep to these rules, and one draw needn't show every extreme that they name: A permutation of the contracts; contract c goes to new block position[c] // 64. Each old block of 64 contracts sends exactly 2 contracts to each of the 32 new blocks.
All inputs are finite; a program needn't handle non-finite values.
Results may differ from the reference program's by a relative error of at most 0.0038.
Values may be sent and summed in bfloat16 or wider, within the bound.
A program may use at most 64 MiB of HBM per device.

```python
import math
import jax
import jax.numpy as jnp
from jax import lax

CAP = 2
LEVELS = 128
SECTIONS = 1
BASIS = 8
ACTIONS = 3
MOVE = 3
CON_DEV = 64
BLOCKS = 32
CONTRACTS = 2048
PATHS = 2048


def draw_position(key, part):
    first_key, second_key, third_key = jax.random.split(jax.random.fold_in(key, 7301), 3)
    groups = CON_DEV // CAP
    offsets = jax.random.permutation(first_key, BLOCKS)[:groups]
    ranking = jax.vmap(lambda sub: jax.random.permutation(sub, CON_DEV))(jax.random.split(second_key, BLOCKS))
    shuffles = jax.vmap(lambda sub: jax.random.permutation(sub, CON_DEV))(jax.random.split(third_key, BLOCKS))
    source_block = jnp.arange(BLOCKS, dtype=jnp.int32)[:, None]
    target = (source_block + offsets[ranking // CAP]) % BLOCKS
    new_slot = shuffles[target, ranking]
    return (target * CON_DEV + new_slot).reshape(-1).astype(jnp.int32)


def set_ends(drawn, rng, low, top_value):
    spot = [jax.random.randint(jax.random.fold_in(rng, axis), (), 0, length) for axis, length in enumerate(drawn.shape)]
    widest = drawn.shape.index(max(drawn.shape))
    neighbour = spot[:widest] + [(spot[widest] + 1) % drawn.shape[widest]] + spot[widest + 1:]
    return drawn.at[tuple(spot)].set(low).at[tuple(neighbour)].set(top_value)


def block_levels(own_key, dims, cuts, least, high):
    loudness = 1.0
    for dim, parts in cuts:
        heights = jax.random.uniform(jax.random.fold_in(jax.random.fold_in(own_key, 6), dim), (parts,), jnp.float32, least / len(cuts), high / len(cuts))
        loudness = loudness * jnp.repeat(jnp.exp(heights), dims[dim] // parts).reshape((-1,) + (1,) * (len(dims) - 1 - dim))
    return loudness


def gaussian(stream_key, dims, scale, limit, cuts=(), held_as=jnp.bfloat16):
    drawn = jax.random.normal(stream_key, dims, jnp.float32) * scale
    if len(cuts) > 0:
        drawn = block_levels(stream_key, dims, cuts, -0.22, 0.18) * drawn
    return jnp.clip(drawn, min=-limit, max=limit).astype(held_as)


def setup_inputs(seed: int = 0) -> dict:
    arg_keys = jax.random.split(jax.random.key(seed), 8)
    prices = gaussian(arg_keys[0], (SECTIONS, PATHS), 1.0, 6.0, ((1, 16),), jnp.float32)
    terminal = gaussian(arg_keys[1], (CONTRACTS, PATHS, LEVELS), 1.0, 6.0, ((0, 32), (1, 16)))
    band = set_ends(jax.random.randint(arg_keys[2], (CONTRACTS,), LEVELS // 4, LEVELS + 1), jax.random.fold_in(arg_keys[2], 1), LEVELS // 4, LEVELS).astype(jnp.int32)
    position = draw_position(jax.random.fold_in(arg_keys[7], 71), 0)
    actions = set_ends(jax.random.randint(arg_keys[4], (CONTRACTS, ACTIONS), -MOVE, MOVE + 1), jax.random.fold_in(arg_keys[4], 1), -MOVE, MOVE).astype(jnp.int32)
    degree = set_ends(jax.random.randint(arg_keys[5], (CONTRACTS,), 2, BASIS), jax.random.fold_in(arg_keys[5], 1), 2, BASIS - 1).astype(jnp.int32)
    volume = jnp.clip(jnp.exp(jax.random.uniform(arg_keys[6], (CONTRACTS,), jnp.float32, math.log(0.05), math.log(0.5))), 0.05, 0.5)
    return {"prices": prices, "terminal": terminal, "band": band, "position": position, "actions": actions, "degree": degree, "volume": volume}


RIDGE = 0.05
DISCOUNT = 0.98
SPOT_SCALE = 0.25

def chebyshev(prices_row):
    scaled = jnp.tanh(prices_row)
    series = [jnp.ones_like(scaled), scaled]
    for order in range(2, BASIS):
        series.append(2.0 * scaled * series[-1] - series[-2])
    return jnp.stack(series[:BASIS])

def regress(gram, moments, path_count, degree_block):
    orders = jnp.arange(BASIS, dtype=jnp.int32)
    keep_basis = (orders[None, :] <= degree_block[:, None]).astype(jnp.float32)
    identity = jnp.eye(BASIS, dtype=jnp.float32)
    system = keep_basis[:, :, None] * keep_basis[:, None, :] * (gram / path_count)[None]
    system = system + (1.0 - keep_basis)[:, :, None] * identity[None] + RIDGE * identity[None]
    scaled_moments = keep_basis[:, :, None] * (moments / path_count)
    factor = jnp.linalg.cholesky(system)
    halfway = lax.linalg.triangular_solve(factor, scaled_moments, left_side=True, lower=True)
    return lax.linalg.triangular_solve(factor, halfway, left_side=True, lower=True, transpose_a=True)

def decide(values_now, estimate, spot_price, band_block, action_block, volume_block):
    levels = jnp.arange(LEVELS, dtype=jnp.int32)
    living = levels[None, :] < band_block[:, None]
    padded = jnp.pad(estimate, ((0, 0), (0, 0), (MOVE, MOVE)))
    optimum = DISCOUNT * estimate
    for offset in range(-MOVE, MOVE + 1):
        if offset == 0:
            continue
        allowed = jnp.any(action_block == offset, axis=1)
        target_level = levels + offset
        inside = (target_level[None, :] >= 0) & (target_level[None, :] < band_block[:, None])
        moved = padded[:, :, MOVE + offset:MOVE + offset + LEVELS]
        candidate = -offset * volume_block[:, None, None] * spot_price[None, :, None] + DISCOUNT * moved
        usable = allowed[:, None, None] & inside[:, None, :]
        optimum = jnp.where(usable, jnp.maximum(optimum, candidate), optimum)
    return jnp.where(living[:, None, :], optimum + DISCOUNT * (values_now - estimate), 0.0)

def reference(prices, terminal, band, position, actions, degree, volume):
    highest = lax.Precision.HIGHEST
    basis_all = jnp.stack([chebyshev(prices[section]) for section in range(SECTIONS)])
    grams = jnp.einsum('skp,sjp->skj', basis_all, basis_all, precision=highest)
    spots = jnp.exp(SPOT_SCALE * prices)
    arrival = jnp.argsort(position).astype(jnp.int32).reshape(CONTRACTS // CON_DEV, CON_DEV)

    def value_block(contract_ids):
        values_now = terminal[contract_ids].astype(jnp.float32)
        band_block = band[contract_ids]
        action_block = actions[contract_ids]
        degree_block = degree[contract_ids]
        volume_block = volume[contract_ids]
        for section in range(SECTIONS - 1, -1, -1):
            moments = jnp.einsum('kp,cpl->ckl', basis_all[section], values_now, precision=highest)
            fitted = regress(grams[section], moments, PATHS, degree_block)
            estimate = jnp.einsum('kp,ckl->cpl', basis_all[section], fitted, precision=highest)
            values_now = decide(values_now, estimate, spots[section], band_block, action_block, volume_block)
        return values_now.astype(jnp.bfloat16)
    return lax.map(value_block, arrival).reshape(CONTRACTS, PATHS, LEVELS)
```

```python
import functools

import jax
import jax.numpy as jnp
from jax import lax
from jax.experimental import pallas as pl
from jax.experimental.pallas import tpu as pltpu
from jax.sharding import PartitionSpec as P

LEVELS = 128
BASIS = 8
OFFSETS = (-3, -2, -1, 1, 2, 3)
RIDGE = 0.05
DISCOUNT = 0.98
SPOT_SCALE = 0.25
Z, X = 8, 4
BLOCKS = Z * X
GROUP = 16
CON = 64
ROWS = len(OFFSETS) * 16
FIRST, SECOND = (4,), (3, 5, 2, 6, 1, 7, 0)
MESH = pl.DeviceIdType.MESH
MIB = 1024 * 1024


def order_kernel(position, order, places, count, sem):
    me = lax.axis_index("contract")
    copy = pltpu.make_async_copy(position, places, sem)
    copy.start()

    def clear(i, carry):
        count[i] = 0
        return carry

    lax.fori_loop(0, BLOCKS, clear, 0)
    copy.wait()

    def enter(i, carry):
        target = lax.shift_right_logical(places[me * CON + i], 6)
        rank = count[target]
        count[target] = rank + 1
        order[2 * target + rank] = i
        return carry

    lax.fori_loop(0, CON, enter, 0, unroll=4)


def split(value):
    high = value.astype(jnp.bfloat16)
    low = (value - high.astype(jnp.float32)).astype(jnp.bfloat16)
    return high, low


def place(block):
    return lax.rem(block, 2) * 16 + block // 2


def exchange_kernel(
    paths,
    prices_in,
    terminal_in,
    order_in,
    position_in,
    band_in,
    degree_in,
    actions_in,
    volume_in,
    arrived,
    gain,
    live,
    slots,
    prices,
    terminal,
    order,
    position,
    band,
    degree,
    actions,
    volume,
    sent,
    partial,
    slab,
    slab_in,
    row_out,
    row_in,
    share,
    moments,
    factor,
    table,
    left,
    params,
    ssem,
    rsem,
    fetch_sem,
):
    me = lax.axis_index("contract")
    mine = lax.axis_index("paths")
    z, x = me // X, lax.rem(me, X)

    def block(dz, dx):
        return lax.rem(z + dz + 2 * Z, Z) * X + lax.rem(x + dx + 2 * X, X)

    barrier = pltpu.get_barrier_semaphore()
    for dz in range(Z):
        for dx in range(X):
            if dz or dx:
                pl.semaphore_signal(barrier, inc=1, device_id=(mine, block(dz, dx)), device_id_type=MESH)
    for d in range(1, GROUP):
        pl.semaphore_signal(barrier, inc=1, device_id=(lax.rem(mine + d, GROUP), me), device_id_type=MESH)
    fetches = [
        pltpu.make_async_copy(src, dst, fetch_sem.at[n])
        for n, (src, dst) in enumerate(
            (
                (terminal_in, terminal),
                (order_in, order),
                (prices_in, prices),
                (position_in, position),
                (band_in, band),
                (degree_in, degree),
                (actions_in, actions),
                (volume_in, volume),
            )
        )
    ]
    for fetch in fetches:
        fetch.start()

    used = [0]
    started = []

    def send(src, dst, device):
        i = used[0]
        used[0] += 1
        copy = pltpu.make_async_remote_copy(
            src_ref=src, dst_ref=dst, send_sem=ssem.at[i], recv_sem=rsem.at[i],
            device_id=device, device_id_type=MESH,
        )
        copy.start()
        started.append(copy)
        return copy

    for fetch in fetches:
        fetch.wait()

    def arrange(i, carry):
        sent[i] = terminal[order[i]]
        return carry

    lax.fori_loop(0, CON, arrange, 0, unroll=2)

    price = prices[...]
    scaled = jnp.tanh(price)
    series = [jnp.ones_like(scaled), scaled]
    for _ in range(2, BASIS):
        series.append(2.0 * scaled * series[-1] - series[-2])
    spot = jnp.exp(SPOT_SCALE * price)
    basis = jnp.concatenate(series, axis=0)
    basis_high, basis_low = split(basis)
    both = jnp.concatenate([basis, spot, jnp.zeros((7, 128), jnp.float32)], axis=0)
    high, low = split(both)
    high, low = high.astype(jnp.float32), low.astype(jnp.float32)
    turned = jnp.transpose(jnp.concatenate([high, high, low, both, jnp.zeros((64, 128), jnp.float32)], axis=0))
    left[...] = turned[:, :48].astype(jnp.bfloat16)
    gram_part = lax.dot_general(
        basis, basis, (((1,), (1,)), ((), ())),
        precision=lax.Precision.HIGHEST, preferred_element_type=jnp.float32,
    )
    gram_part = jnp.concatenate([gram_part, jnp.zeros((BASIS, 120), jnp.float32)], axis=1)

    pl.semaphore_wait(barrier, BLOCKS - 1 + GROUP - 1)

    def pair(where):
        return pl.ds(2 * where, 2)

    grids = []

    def send_grids(shifts):
        for dz in shifts:
            for dx in range(X):
                if dz or dx:
                    to = block(dz, dx)
                    grids.append(send(sent.at[pair(to)], arrived.at[pair(place(me))], (mine, to)))

    send_grids(FIRST)

    basis_both = jnp.concatenate([basis_high, basis_low], axis=0)

    def one_target(t, carry):
        two = jnp.concatenate([sent[2 * t], sent[2 * t + 1]], axis=1)
        result = jnp.dot(basis_both, two, preferred_element_type=jnp.float32)
        result = result[:BASIS] + result[BASIS:]
        start = pl.multiple_of(16 * t, 16)
        partial[pl.ds(start, 8), :] = result[:, :128]
        partial[pl.ds(start + 8, 8), :] = result[:, 128:]
        return carry

    lax.fori_loop(0, BLOCKS, one_target, 0, unroll=4)
    for q in range(GROUP):
        slab[q, 0:32, :] = partial[pl.ds(q, 32, stride=16), :]
        slab[q, 32:40, :] = gram_part
    shares = []
    for d in range(1, GROUP):
        q = lax.rem(mine + d, GROUP)
        shares.append(send(slab.at[q], slab_in.at[mine], (q, me)))
    slab_in[mine] = slab[mine]
    table[...] = jnp.zeros_like(table)
    arrived[pair(place(me))] = sent[pair(me)]

    lane = lax.broadcasted_iota(jnp.int32, (16, 128), 1)
    lane_f = lane.astype(jnp.float32)
    places = position[...]
    low_bits = (places + lax.shift_left(band[...], 11) + lax.shift_left(degree[...], 19)).astype(jnp.float32)
    allowed = jnp.zeros((16, 128), jnp.int32)
    for a in range(3):
        moves = jnp.concatenate([actions[a : a + 1, 128 * row : 128 * row + 128] for row in range(16)], axis=0)
        for n, offset in enumerate(OFFSETS):
            allowed = jnp.bitwise_or(allowed, jnp.where(moves == offset, 1 << n, 0))
    high_bits = allowed.astype(jnp.float32)
    volumes = volume[...]
    target = lax.shift_right_logical(places, 6)
    for h in range(2):
        here = (target == me) & ((lane >= 64) if h else (lane < 64))
        first = jnp.min(jnp.where(here, lane_f, 1000.0), axis=1, keepdims=True)
        last = jnp.max(jnp.where(here, lane_f, -1.0), axis=1, keepdims=True)
        for r, index in enumerate((first, last)):
            chosen = lane_f == index
            for n, value in enumerate((low_bits, high_bits, volumes)):
                total = jnp.sum(jnp.where(chosen, value, 0.0), axis=1, keepdims=True)
                params[n, r, 16 * h : 16 * h + 16, :] = jnp.broadcast_to(total, (16, 128))
    lane32 = lax.broadcasted_iota(jnp.int32, (32, 128), 1)
    row32 = lax.broadcasted_iota(jnp.int32, (32, 128), 0)
    slot_row = jnp.zeros((1, 128), jnp.float32)
    for r in range(2):
        word = params[0, r].astype(jnp.int32)
        levels = jnp.bitwise_and(lax.shift_right_logical(word, 11), 255)
        live[r] = jnp.where(lane32 < levels, DISCOUNT, 0.0)
        slot = jnp.bitwise_and(word, 63).astype(jnp.float32)
        slot_row = slot_row + jnp.sum(jnp.where(lane32 == row32 + 32 * r, slot, 0.0), axis=0, keepdims=True)
    slots[...] = slot_row.astype(jnp.int32)

    for copy in shares:
        copy.wait_recv()
    total = slab_in[0]
    for q in range(1, GROUP):
        total = total + slab_in[q]
    row_out[...] = total[0:32].reshape(32, 1, 128)
    row_in[place(me)] = row_out[me]
    small = []
    for dz in range(Z):
        for dx in range(X):
            if dz or dx:
                to = block(dz, dx)
                small.append(send(row_out.at[to], row_in.at[place(me)], (mine, to)))
    send_grids(SECOND)

    eye = lax.broadcasted_iota(jnp.int32, (8, 128), 0) == lax.broadcasted_iota(jnp.int32, (8, 128), 1)
    system = total[32:40] / float(paths) + jnp.where(eye, RIDGE, 0.0)
    slot_of = {}
    for j in range(BASIS):
        inverse = 1.0 / jnp.sqrt(system[j : j + 1, j : j + 1])
        column = system[:, j : j + 1] * inverse
        across = system[j : j + 1, :] * inverse
        system = system - column * across
        slot_of[j, j] = len(slot_of)
        factor[slot_of[j, j]] = jnp.broadcast_to(inverse, (8, 128))
        for i in range(j + 1, BASIS):
            slot_of[i, j] = len(slot_of)
            factor[slot_of[i, j]] = jnp.broadcast_to(column[i : i + 1, :], (8, 128))

    for copy in small:
        copy.wait_recv()
    share[...] = row_in[...].reshape(32, 128)
    moments[mine] = share[...]
    gathers = []
    for d in range(1, GROUP):
        q = lax.rem(mine + d, GROUP)
        gathers.append(send(share, moments.at[mine], (q, me)))

    for copy in gathers:
        copy.wait_recv()
    lane8 = lax.broadcasted_iota(jnp.int32, (8, 128), 1)
    for tile in range(4):
        rows = slice(8 * tile, 8 * tile + 8)
        for r in range(2):
            word = params[0, r, rows, :].astype(jnp.int32)
            moves = params[1, r, rows, :].astype(jnp.int32)
            vol = params[2, r, rows, :]
            levels = jnp.bitwise_and(lax.shift_right_logical(word, 11), 255)
            highest = lax.shift_right_logical(word, 19)
            halfway, fitted = [], [None] * BASIS
            for i in range(BASIS):
                value = moments[8 * r + i, rows, :] / float(paths)
                for j in range(i):
                    value = value - factor[slot_of[i, j]] * halfway[j]
                halfway.append(value * factor[slot_of[i, i]])
            for i in reversed(range(BASIS)):
                value = halfway[i]
                for j in range(i + 1, BASIS):
                    value = value - factor[slot_of[j, i]] * fitted[j]
                fitted[i] = jnp.where(highest >= i, value * factor[slot_of[i, i]], 0.0)
            first = (16 * tile + r) * ROWS
            for n, offset in enumerate(OFFSETS):
                bit = jnp.bitwise_and(lax.shift_right_logical(moves, n), 1)
                to = lane8 + offset
                usable = (bit == 1) & (to >= 0) & (to < levels) & (lane8 < levels)
                for k in range(BASIS):
                    moved = pltpu.roll(fitted[k], (-offset) % LEVELS, 1)
                    table[pl.ds(first + 16 * n + k, 8, stride=2 * ROWS), :] = jnp.where(
                        usable, DISCOUNT * (moved - fitted[k]), 0.0
                    )
                table[pl.ds(first + 16 * n + BASIS, 8, stride=2 * ROWS), :] = jnp.where(
                    usable, -float(offset) * vol, 0.0
                )

    def best(c, carry):
        rows = table[pl.ds(pl.multiple_of(c * ROWS, 16), ROWS), :]
        value = jnp.zeros((128, 128), jnp.float32)
        for n in range(0, len(OFFSETS), 2):
            two = jnp.concatenate([rows[16 * n : 16 * n + 16], rows[16 * n + 16 : 16 * n + 32]], axis=1)
            two_high, two_low = split(two)
            right = jnp.concatenate([two_high, two_low, two_high], axis=0)
            result = jnp.dot(left[...], right, preferred_element_type=jnp.float32)
            value = jnp.maximum(value, jnp.maximum(result[:, :128], result[:, 128:]))
        gain[c] = value
        return carry

    lax.fori_loop(0, CON, best, 0, unroll=2)
    for copy in grids:
        copy.wait_recv()
    for copy in started:
        copy.wait_send()


SENDS = 2 * (BLOCKS - 1) + 2 * (GROUP - 1)


def finish_kernel(slots, arrived, gain, live, valued, ready, sem):
    for r in range(2):

        def one(row, carry):
            c = 2 * row + r
            kept = live[r, pl.ds(row, 1), :]
            ready[c] = (gain[c] + kept * arrived[c].astype(jnp.float32)).astype(jnp.bfloat16)
            pltpu.make_async_copy(ready.at[c], valued.at[slots[0, 32 * r + row]], sem).start()
            return carry

        lax.fori_loop(0, BLOCKS, one, 0)
    pltpu.make_async_copy(ready, valued, sem).wait()


def in_vmem(array):
    return pltpu.with_memory_space_constraint(array, pltpu.VMEM)


def kept_in_hbm(array):
    return pltpu.with_memory_space_constraint(array, pltpu.HBM)


def per_device(prices, terminal, band, position, actions, degree, volume):
    paths = prices.shape[1] * lax.axis_size("paths")
    con, width, levels = terminal.shape
    vmem = pl.BlockSpec(memory_space=pltpu.VMEM)
    anywhere = pl.BlockSpec(memory_space=pl.ANY)
    in_hbm = pl.BlockSpec(memory_space=pltpu.HBM)
    scalars = pl.BlockSpec(memory_space=pltpu.SMEM)
    grids = (con, width, levels)

    def table(array):
        return array.reshape(16, 128)

    order = pl.pallas_call(
        order_kernel,
        out_shape=jax.ShapeDtypeStruct((CON,), jnp.int32),
        in_specs=[in_hbm],
        out_specs=scalars,
        scratch_shapes=[
            pltpu.SMEM((CON * BLOCKS,), jnp.int32),
            pltpu.SMEM((BLOCKS,), jnp.int32),
            pltpu.SemaphoreType.DMA,
        ],
        compiler_params=pltpu.CompilerParams(vmem_limit_bytes=8 * MIB),
        name="order",
    )(kept_in_hbm(position))

    dma = pltpu.SemaphoreType.DMA
    f32, bf16 = jnp.float32, jnp.bfloat16
    arrived, gain, live, slots = pl.pallas_call(
        functools.partial(exchange_kernel, paths),
        out_shape=(
            pltpu.VMEM(grids, bf16),
            pltpu.VMEM(grids, f32),
            pltpu.VMEM((2, 32, 128), f32),
            jax.ShapeDtypeStruct((1, 128), jnp.int32),
        ),
        in_specs=[in_hbm] * 8,
        out_specs=(vmem,) * 4,
        scratch_shapes=[
            pltpu.VMEM((1, width), f32),
            pltpu.VMEM(grids, bf16),
            pltpu.SMEM((CON,), jnp.int32),
            pltpu.VMEM((16, 128), jnp.int32),
            pltpu.VMEM((16, 128), jnp.int32),
            pltpu.VMEM((16, 128), jnp.int32),
            pltpu.VMEM((3, 2048), jnp.int32),
            pltpu.VMEM((16, 128), f32),
            pltpu.VMEM(grids, bf16),
            pltpu.VMEM((512, 128), f32),
            pltpu.VMEM((GROUP, 40, 128), f32),
            pltpu.VMEM((GROUP, 40, 128), f32),
            pltpu.VMEM((32, 1, 128), f32),
            pltpu.VMEM((32, 1, 128), f32),
            pltpu.VMEM((32, 128), f32),
            pltpu.VMEM((GROUP, 32, 128), f32),
            pltpu.VMEM((36, 8, 128), f32),
            pltpu.VMEM((CON * ROWS, 128), f32),
            pltpu.VMEM((128, 48), bf16),
            pltpu.VMEM((3, 2, 32, 128), f32),
            dma((SENDS,)),
            dma((SENDS,)),
            dma((8,)),
        ],
        compiler_params=pltpu.CompilerParams(
            collective_id=0, has_side_effects=True, vmem_limit_bytes=24 * MIB
        ),
        name="exchange",
    )(
        *map(kept_in_hbm, (prices, terminal)),
        order,
        *map(kept_in_hbm, (*map(table, (position, band, degree)), actions.T, table(volume))),
    )

    return pl.pallas_call(
        finish_kernel,
        out_shape=jax.ShapeDtypeStruct(grids, bf16),
        in_specs=[scalars, vmem, vmem, vmem],
        out_specs=anywhere,
        scratch_shapes=[pltpu.VMEM(grids, bf16), dma],
        compiler_params=pltpu.CompilerParams(vmem_limit_bytes=16 * MIB),
        name="finish",
    )(slots, in_vmem(arrived), in_vmem(gain), in_vmem(live))


def solution(mesh):
    in_specs = (P(None, "paths"), P("contract", "paths", None), P(), P(), P(), P(), P())
    return jax.shard_map(
        per_device, mesh=mesh, in_specs=in_specs, out_specs=P("contract", "paths", None), check_vma=False
    )
```

```python
import functools

import jax
import jax.numpy as jnp
from jax import lax
from jax.experimental import pallas as pl
from jax.experimental.pallas import tpu as pltpu
from jax.sharding import PartitionSpec as P

LEVELS = 128
BASIS = 8
OFFSETS = (-3, -2, -1, 1, 2, 3)
RIDGE = 0.05
DISCOUNT = 0.98
SPOT_SCALE = 0.25
Z, X = 8, 4
BLOCKS = Z * X
GROUP = 16
CON = 64
ROWS = len(OFFSETS) * 16
FIRST, SECOND, THIRD = (4,), (3, 5, 2), (6, 1, 7, 0)
MESH = pl.DeviceIdType.MESH
MIB = 1024 * 1024


def split(value):
    high = value.astype(jnp.bfloat16)
    low = (value - high.astype(jnp.float32)).astype(jnp.bfloat16)
    return high, low


def place(block):
    return lax.rem(block, 2) * 16 + block // 2


def exchange_kernel(
    paths,
    prices_in,
    terminal_in,
    position_in,
    band_in,
    degree_in,
    actions_in,
    volume_in,
    arrived,
    gain,
    live,
    slots,
    prices,
    terminal,
    order_row,
    order,
    position,
    band,
    degree,
    actions,
    volume,
    sent,
    partial,
    slab,
    slab_in,
    row_out,
    row_mid,
    row_in,
    share,
    moments,
    factor,
    table,
    left,
    params,
    ssem,
    rsem,
    fetch_sem,
):
    me = lax.axis_index("contract")
    mine = lax.axis_index("paths")
    z, x = me // X, lax.rem(me, X)

    def block(dz, dx):
        return lax.rem(z + dz + 2 * Z, Z) * X + lax.rem(x + dx + 2 * X, X)

    barrier = pltpu.get_barrier_semaphore()
    for dz in range(Z):
        for dx in range(X):
            if dz or dx:
                pl.semaphore_signal(barrier, inc=1, device_id=(mine, block(dz, dx)), device_id_type=MESH)
    for d in range(1, GROUP):
        pl.semaphore_signal(barrier, inc=1, device_id=(lax.rem(mine + d, GROUP), me), device_id_type=MESH)
    fetches = [
        pltpu.make_async_copy(src, dst, fetch_sem.at[n])
        for n, (src, dst) in enumerate(
            (
                (terminal_in, terminal),
                (prices_in, prices),
                (position_in, position),
                (band_in, band),
                (degree_in, degree),
                (actions_in, actions),
                (volume_in, volume),
            )
        )
    ]
    for fetch in fetches:
        fetch.start()

    used = [0]
    started = []

    def send(src, dst, device):
        i = used[0]
        used[0] += 1
        copy = pltpu.make_async_remote_copy(
            src_ref=src, dst_ref=dst, send_sem=ssem.at[i], recv_sem=rsem.at[i],
            device_id=device, device_id_type=MESH,
        )
        copy.start()
        started.append(copy)
        return copy

    for fetch in fetches[1:]:
        fetch.wait()
    lane32 = lax.broadcasted_iota(jnp.int32, (32, 128), 1)
    row32 = lax.broadcasted_iota(jnp.int32, (32, 128), 0)
    half = lax.rem(me, 2) * 64
    own = lax.shift_right_logical(position[pl.ds(me // 2, 1), :], 6)
    going = (own == row32) & (lane32 >= half) & (lane32 < half + 64)
    within = (lane32 - half).astype(jnp.float32)
    first = jnp.min(jnp.where(going, within, 1000.0), axis=1, keepdims=True)
    last = jnp.max(jnp.where(going, within, -1.0), axis=1, keepdims=True)
    picked = jnp.where(lane32 == row32, first, 0.0) + jnp.where(lane32 == row32 + 32, last, 0.0)
    picked = jnp.clip(jnp.sum(picked, axis=0, keepdims=True), 0.0, CON - 1.0)
    order_row[...] = picked.astype(jnp.int32)

    price = prices[...]
    scaled = jnp.tanh(price)
    series = [jnp.ones_like(scaled), scaled]
    for _ in range(2, BASIS):
        series.append(2.0 * scaled * series[-1] - series[-2])
    spot = jnp.exp(SPOT_SCALE * price)
    basis = jnp.concatenate(series, axis=0)
    basis_high, basis_low = split(basis)
    ordered = pltpu.make_async_copy(order_row, order, fetch_sem.at[7])
    ordered.start()
    both = jnp.concatenate([basis, spot, jnp.zeros((7, 128), jnp.float32)], axis=0)
    high, low = split(both)
    high, low = high.astype(jnp.float32), low.astype(jnp.float32)
    turned = jnp.transpose(jnp.concatenate([high, high, low, both, jnp.zeros((64, 128), jnp.float32)], axis=0))
    left[...] = turned[:, :48].astype(jnp.bfloat16)
    gram_part = lax.dot_general(
        basis, basis, (((1,), (1,)), ((), ())),
        precision=lax.Precision.HIGHEST, preferred_element_type=jnp.float32,
    )
    gram_part = jnp.concatenate([gram_part, jnp.zeros((BASIS, 120), jnp.float32)], axis=1)

    ordered.wait()
    fetches[0].wait()

    def arrange(t, carry):
        sent[2 * t] = terminal[jnp.bitwise_and(order[0, t], CON - 1)]
        sent[2 * t + 1] = terminal[jnp.bitwise_and(order[0, BLOCKS + t], CON - 1)]
        return carry

    lax.fori_loop(0, BLOCKS, arrange, 0)

    pl.semaphore_wait(barrier, BLOCKS - 1 + GROUP - 1)

    def pair(where):
        return pl.ds(2 * where, 2)

    grids = []

    def send_grids(shifts):
        for dz in shifts:
            for dx in range(X):
                if dz or dx:
                    to = block(dz, dx)
                    grids.append(send(sent.at[pair(to)], arrived.at[pair(place(me))], (mine, to)))

    send_grids(FIRST)

    basis_both = jnp.concatenate([basis_high, basis_low], axis=0)

    def one_target(t, carry):
        two = jnp.concatenate([sent[2 * t], sent[2 * t + 1]], axis=1)
        result = jnp.dot(basis_both, two, preferred_element_type=jnp.float32)
        result = result[:BASIS] + result[BASIS:]
        start = pl.multiple_of(16 * t, 16)
        partial[pl.ds(start, 8), :] = result[:, :128]
        partial[pl.ds(start + 8, 8), :] = result[:, 128:]
        return carry

    lax.fori_loop(0, BLOCKS, one_target, 0, unroll=4)
    for q in range(GROUP):
        slab[q, 0:32, :] = partial[pl.ds(q, 32, stride=16), :]
        slab[q, 32:40, :] = gram_part
    shares = []
    for d in range(1, GROUP):
        q = lax.rem(mine + d, GROUP)
        shares.append(send(slab.at[q], slab_in.at[mine], (q, me)))
    slab_in[mine] = slab[mine]
    table[...] = jnp.zeros_like(table)
    arrived[pair(place(me))] = sent[pair(me)]

    lane = lax.broadcasted_iota(jnp.int32, (16, 128), 1)
    lane_f = lane.astype(jnp.float32)
    places = position[...]
    low_bits = (places + lax.shift_left(band[...], 11) + lax.shift_left(degree[...], 19)).astype(jnp.float32)
    allowed = jnp.zeros((16, 128), jnp.int32)
    for a in range(3):
        moves = jnp.concatenate([actions[a : a + 1, 128 * row : 128 * row + 128] for row in range(16)], axis=0)
        for n, offset in enumerate(OFFSETS):
            allowed = jnp.bitwise_or(allowed, jnp.where(moves == offset, 1 << n, 0))
    high_bits = allowed.astype(jnp.float32)
    volumes = volume[...]
    target = lax.shift_right_logical(places, 6)
    for h in range(2):
        here = (target == me) & ((lane >= 64) if h else (lane < 64))
        first = jnp.min(jnp.where(here, lane_f, 1000.0), axis=1, keepdims=True)
        last = jnp.max(jnp.where(here, lane_f, -1.0), axis=1, keepdims=True)
        for r, index in enumerate((first, last)):
            chosen = lane_f == index
            for n, value in enumerate((low_bits, high_bits, volumes)):
                total = jnp.sum(jnp.where(chosen, value, 0.0), axis=1, keepdims=True)
                params[n, r, 16 * h : 16 * h + 16, :] = jnp.broadcast_to(total, (16, 128))
    slot_row = jnp.zeros((1, 128), jnp.float32)
    for r in range(2):
        word = params[0, r].astype(jnp.int32)
        levels = jnp.bitwise_and(lax.shift_right_logical(word, 11), 255)
        live[r] = jnp.where(lane32 < levels, DISCOUNT, 0.0)
        slot = jnp.bitwise_and(word, 63).astype(jnp.float32)
        slot_row = slot_row + jnp.sum(jnp.where(lane32 == row32 + 32 * r, slot, 0.0), axis=0, keepdims=True)
    slots[...] = slot_row.astype(jnp.int32)

    for copy in shares:
        copy.wait_recv()
    total = slab_in[0]
    for q in range(1, GROUP):
        total = total + slab_in[q]
    for zz in range(Z):
        row_out[zz] = total[X * zz : X * zz + X].reshape(X, 1, 128)
    row_mid[z] = row_out[z]
    small_z = []
    for dz in range(1, Z):
        small_z.append(send(row_out.at[lax.rem(z + dz, Z)], row_mid.at[z], (mine, block(dz, 0))))
    send_grids(SECOND)

    eye = lax.broadcasted_iota(jnp.int32, (8, 128), 0) == lax.broadcasted_iota(jnp.int32, (8, 128), 1)
    system = total[32:40] / float(paths) + jnp.where(eye, RIDGE, 0.0)
    slot_of = {}
    for j in range(BASIS):
        inverse = 1.0 / jnp.sqrt(system[j : j + 1, j : j + 1])
        column = system[:, j : j + 1] * inverse
        across = system[j : j + 1, :] * inverse
        system = system - column * across
        slot_of[j, j] = len(slot_of)
        factor[slot_of[j, j]] = jnp.broadcast_to(inverse, (8, 128))
        for i in range(j + 1, BASIS):
            slot_of[i, j] = len(slot_of)
            factor[slot_of[i, j]] = jnp.broadcast_to(column[i : i + 1, :], (8, 128))

    for copy in small_z:
        copy.wait_recv()
    row_in[x] = row_mid[:, x]
    small_x = []
    for dx in range(1, X):
        small_x.append(send(row_mid.at[:, lax.rem(x + dx, X)], row_in.at[x], (mine, block(0, dx))))
    send_grids(THIRD)
    for copy in small_x:
        copy.wait_recv()
    for xx in range(X):
        share[pl.ds(16 * (xx % 2) + xx // 2, Z, stride=2), :] = row_in[xx].reshape(Z, 128)
    moments[mine] = share[...]
    gathers = []
    for d in range(1, GROUP):
        q = lax.rem(mine + d, GROUP)
        gathers.append(send(share, moments.at[mine], (q, me)))

    for copy in gathers:
        copy.wait_recv()
    lane8 = lax.broadcasted_iota(jnp.int32, (8, 128), 1)
    for tile in range(4):
        rows = slice(8 * tile, 8 * tile + 8)
        for r in range(2):
            word = params[0, r, rows, :].astype(jnp.int32)
            moves = params[1, r, rows, :].astype(jnp.int32)
            vol = params[2, r, rows, :]
            levels = jnp.bitwise_and(lax.shift_right_logical(word, 11), 255)
            highest = lax.shift_right_logical(word, 19)
            halfway, fitted = [], [None] * BASIS
            for i in range(BASIS):
                value = moments[8 * r + i, rows, :] / float(paths)
                for j in range(i):
                    value = value - factor[slot_of[i, j]] * halfway[j]
                halfway.append(value * factor[slot_of[i, i]])
            for i in reversed(range(BASIS)):
                value = halfway[i]
                for j in range(i + 1, BASIS):
                    value = value - factor[slot_of[j, i]] * fitted[j]
                fitted[i] = jnp.where(highest >= i, value * factor[slot_of[i, i]], 0.0)
            first = (16 * tile + r) * ROWS
            for n, offset in enumerate(OFFSETS):
                bit = jnp.bitwise_and(lax.shift_right_logical(moves, n), 1)
                to = lane8 + offset
                usable = (bit == 1) & (to >= 0) & (to < levels) & (lane8 < levels)
                for k in range(BASIS):
                    moved = pltpu.roll(fitted[k], (-offset) % LEVELS, 1)
                    table[pl.ds(first + 16 * n + k, 8, stride=2 * ROWS), :] = jnp.where(
                        usable, DISCOUNT * (moved - fitted[k]), 0.0
                    )
                table[pl.ds(first + 16 * n + BASIS, 8, stride=2 * ROWS), :] = jnp.where(
                    usable, -float(offset) * vol, 0.0
                )

    def best(c, carry):
        rows = table[pl.ds(pl.multiple_of(c * ROWS, 16), ROWS), :]
        value = jnp.zeros((128, 128), jnp.float32)
        for n in range(0, len(OFFSETS), 2):
            two = jnp.concatenate([rows[16 * n : 16 * n + 16], rows[16 * n + 16 : 16 * n + 32]], axis=1)
            two_high, two_low = split(two)
            right = jnp.concatenate([two_high, two_low, two_high], axis=0)
            result = jnp.dot(left[...], right, preferred_element_type=jnp.float32)
            value = jnp.maximum(value, jnp.maximum(result[:, :128], result[:, 128:]))
        gain[c] = value
        return carry

    lax.fori_loop(0, CON, best, 0, unroll=2)
    for copy in grids:
        copy.wait_recv()
    for copy in started:
        copy.wait_send()


SENDS = BLOCKS - 1 + Z - 1 + X - 1 + 2 * (GROUP - 1)


def finish_kernel(slots, arrived, gain, live, valued, ready, sem):
    for r in range(2):

        def one(row, carry):
            c = 2 * row + r
            kept = live[r, pl.ds(row, 1), :]
            ready[c] = (gain[c] + kept * arrived[c].astype(jnp.float32)).astype(jnp.bfloat16)
            pltpu.make_async_copy(ready.at[c], valued.at[slots[0, 32 * r + row]], sem).start()
            return carry

        lax.fori_loop(0, BLOCKS, one, 0)
    pltpu.make_async_copy(ready, valued, sem).wait()


def in_vmem(array):
    return pltpu.with_memory_space_constraint(array, pltpu.VMEM)


def kept_in_hbm(array):
    return pltpu.with_memory_space_constraint(array, pltpu.HBM)


def per_device(prices, terminal, band, position, actions, degree, volume):
    paths = prices.shape[1] * lax.axis_size("paths")
    con, width, levels = terminal.shape
    vmem = pl.BlockSpec(memory_space=pltpu.VMEM)
    anywhere = pl.BlockSpec(memory_space=pl.ANY)
    in_hbm = pl.BlockSpec(memory_space=pltpu.HBM)
    scalars = pl.BlockSpec(memory_space=pltpu.SMEM)
    grids = (con, width, levels)

    def table(array):
        return array.reshape(16, 128)

    dma = pltpu.SemaphoreType.DMA
    f32, bf16 = jnp.float32, jnp.bfloat16
    arrived, gain, live, slots = pl.pallas_call(
        functools.partial(exchange_kernel, paths),
        out_shape=(
            pltpu.VMEM(grids, bf16),
            pltpu.VMEM(grids, f32),
            pltpu.VMEM((2, 32, 128), f32),
            jax.ShapeDtypeStruct((1, 128), jnp.int32),
        ),
        in_specs=[in_hbm] * 7,
        out_specs=(vmem,) * 4,
        scratch_shapes=[
            pltpu.VMEM((1, width), f32),
            pltpu.VMEM(grids, bf16),
            pltpu.VMEM((1, 128), jnp.int32),
            pltpu.SMEM((1, 128), jnp.int32),
            pltpu.VMEM((16, 128), jnp.int32),
            pltpu.VMEM((16, 128), jnp.int32),
            pltpu.VMEM((16, 128), jnp.int32),
            pltpu.VMEM((3, 2048), jnp.int32),
            pltpu.VMEM((16, 128), f32),
            pltpu.VMEM(grids, bf16),
            pltpu.VMEM((512, 128), f32),
            pltpu.VMEM((GROUP, 40, 128), f32),
            pltpu.VMEM((GROUP, 40, 128), f32),
            pltpu.VMEM((Z, X, 1, 128), f32),
            pltpu.VMEM((Z, X, 1, 128), f32),
            pltpu.VMEM((X, Z, 1, 128), f32),
            pltpu.VMEM((32, 128), f32),
            pltpu.VMEM((GROUP, 32, 128), f32),
            pltpu.VMEM((36, 8, 128), f32),
            pltpu.VMEM((CON * ROWS, 128), f32),
            pltpu.VMEM((128, 48), bf16),
            pltpu.VMEM((3, 2, 32, 128), f32),
            dma((SENDS,)),
            dma((SENDS,)),
            dma((8,)),
        ],
        compiler_params=pltpu.CompilerParams(
            collective_id=0, has_side_effects=True, vmem_limit_bytes=24 * MIB
        ),
        name="exchange",
    )(
        *map(kept_in_hbm, (prices, terminal)),
        *map(kept_in_hbm, (*map(table, (position, band, degree)), actions.T, table(volume))),
    )

    return pl.pallas_call(
        finish_kernel,
        out_shape=jax.ShapeDtypeStruct(grids, bf16),
        in_specs=[scalars, vmem, vmem, vmem],
        out_specs=anywhere,
        scratch_shapes=[pltpu.VMEM(grids, bf16), dma],
        compiler_params=pltpu.CompilerParams(vmem_limit_bytes=16 * MIB),
        name="finish",
    )(slots, in_vmem(arrived), in_vmem(gain), in_vmem(live))


def solution(mesh):
    in_specs = (P(None, "paths"), P("contract", "paths", None), P(), P(), P(), P(), P())
    return jax.shard_map(
        per_device, mesh=mesh, in_specs=in_specs, out_specs=P("contract", "paths", None), check_vma=False
    )
```

```python
import functools

import jax
import jax.numpy as jnp
from jax import lax
from jax.experimental import pallas as pl
from jax.experimental.pallas import tpu as pltpu
from jax.sharding import PartitionSpec as P

LEVELS = 128
BASIS = 8
OFFSETS = (-3, -2, -1, 1, 2, 3)
RIDGE = 0.05
DISCOUNT = 0.98
SPOT_SCALE = 0.25
Z, X = 8, 4
BLOCKS = Z * X
GROUP = 16
CON = 64
ROWS = len(OFFSETS) * 16
FIRST, SECOND, THIRD = (4, 0), (3, 5, 2), (6, 1, 7)
MESH = pl.DeviceIdType.MESH
MIB = 1024 * 1024


def split(value):
    high = value.astype(jnp.bfloat16)
    low = (value - high.astype(jnp.float32)).astype(jnp.bfloat16)
    return high, low


def place(block):
    return lax.rem(block, 2) * 16 + block // 2


def exchange_kernel(
    paths,
    prices_in,
    terminal_in,
    position_in,
    band_in,
    degree_in,
    actions_in,
    volume_in,
    arrived,
    gain,
    live,
    slots,
    prices,
    terminal,
    order_row,
    order,
    position,
    band,
    degree,
    actions,
    volume,
    sent,
    partial,
    slab,
    slab_in,
    row_out,
    row_mid,
    row_in,
    share,
    moments,
    factor,
    table,
    left,
    params,
    ssem,
    rsem,
    fetch_sem,
):
    me = lax.axis_index("contract")
    mine = lax.axis_index("paths")
    z, x = me // X, lax.rem(me, X)

    def block(dz, dx):
        return lax.rem(z + dz + 2 * Z, Z) * X + lax.rem(x + dx + 2 * X, X)

    barrier = pltpu.get_barrier_semaphore()
    for dz in range(Z):
        for dx in range(X):
            if dz or dx:
                pl.semaphore_signal(barrier, inc=1, device_id=(mine, block(dz, dx)), device_id_type=MESH)
    for d in range(1, GROUP):
        pl.semaphore_signal(barrier, inc=1, device_id=(lax.rem(mine + d, GROUP), me), device_id_type=MESH)
    fetches = [
        pltpu.make_async_copy(src, dst, fetch_sem.at[n])
        for n, (src, dst) in enumerate(
            (
                (terminal_in, terminal),
                (prices_in, prices),
                (position_in, position),
                (band_in, band),
                (degree_in, degree),
                (actions_in, actions),
                (volume_in, volume),
            )
        )
    ]
    for fetch in fetches:
        fetch.start()

    used = [0]
    started = []

    def send(src, dst, device):
        i = used[0]
        used[0] += 1
        copy = pltpu.make_async_remote_copy(
            src_ref=src, dst_ref=dst, send_sem=ssem.at[i], recv_sem=rsem.at[i],
            device_id=device, device_id_type=MESH,
        )
        copy.start()
        started.append(copy)
        return copy

    for fetch in fetches[1:]:
        fetch.wait()
    lane32 = lax.broadcasted_iota(jnp.int32, (32, 128), 1)
    row32 = lax.broadcasted_iota(jnp.int32, (32, 128), 0)
    half = lax.rem(me, 2) * 64
    own = lax.shift_right_logical(position[pl.ds(me // 2, 1), :], 6)
    going = (own == row32) & (lane32 >= half) & (lane32 < half + 64)
    within = (lane32 - half).astype(jnp.float32)
    first = jnp.min(jnp.where(going, within, 1000.0), axis=1, keepdims=True)
    last = jnp.max(jnp.where(going, within, -1.0), axis=1, keepdims=True)
    picked = jnp.where(lane32 == row32, first, 0.0) + jnp.where(lane32 == row32 + 32, last, 0.0)
    picked = jnp.clip(jnp.sum(picked, axis=0, keepdims=True), 0.0, CON - 1.0)
    order_row[...] = picked.astype(jnp.int32)

    price = prices[...]
    scaled = jnp.tanh(price)
    series = [jnp.ones_like(scaled), scaled]
    for _ in range(2, BASIS):
        series.append(2.0 * scaled * series[-1] - series[-2])
    spot = jnp.exp(SPOT_SCALE * price)
    basis = jnp.concatenate(series, axis=0)
    basis_high, basis_low = split(basis)
    ordered = pltpu.make_async_copy(order_row, order, fetch_sem.at[7])
    ordered.start()
    both = jnp.concatenate([basis, spot, jnp.zeros((7, 128), jnp.float32)], axis=0)
    high, low = split(both)
    high, low = high.astype(jnp.float32), low.astype(jnp.float32)
    turned = jnp.transpose(jnp.concatenate([high, high, low, both, jnp.zeros((64, 128), jnp.float32)], axis=0))
    left[...] = turned[:, :48].astype(jnp.bfloat16)
    gram_part = lax.dot_general(
        basis, basis, (((1,), (1,)), ((), ())),
        precision=lax.Precision.HIGHEST, preferred_element_type=jnp.float32,
    )
    gram_part = jnp.concatenate([gram_part, jnp.zeros((BASIS, 120), jnp.float32)], axis=1)

    ordered.wait()
    fetches[0].wait()

    def arrange(t, carry):
        sent[2 * t] = terminal[jnp.bitwise_and(order[0, t], CON - 1)]
        sent[2 * t + 1] = terminal[jnp.bitwise_and(order[0, BLOCKS + t], CON - 1)]
        return carry

    lax.fori_loop(0, BLOCKS, arrange, 0)

    pl.semaphore_wait(barrier, BLOCKS - 1 + GROUP - 1)

    def pair(where):
        return pl.ds(2 * where, 2)

    grids = []

    def send_grids(shifts):
        for dx in (2, 1, 3, 0):
            for dz in shifts:
                if dz or dx:
                    to = block(dz, dx)
                    grids.append(send(sent.at[pair(to)], arrived.at[pair(place(me))], (mine, to)))

    send_grids(FIRST)

    basis_both = jnp.concatenate([basis_high, basis_low], axis=0)

    def one_target(t, carry):
        two = jnp.concatenate([sent[2 * t], sent[2 * t + 1]], axis=1)
        result = jnp.dot(basis_both, two, preferred_element_type=jnp.float32)
        result = result[:BASIS] + result[BASIS:]
        start = pl.multiple_of(16 * t, 16)
        partial[pl.ds(start, 8), :] = result[:, :128]
        partial[pl.ds(start + 8, 8), :] = result[:, 128:]
        return carry

    lax.fori_loop(0, BLOCKS, one_target, 0, unroll=4)
    for q in range(GROUP):
        slab[q, 0:32, :] = partial[pl.ds(q, 32, stride=16), :]
        slab[q, 32:40, :] = gram_part
    shares = []
    for d in range(1, GROUP):
        q = lax.rem(mine + d, GROUP)
        shares.append(send(slab.at[q], slab_in.at[mine], (q, me)))
    slab_in[mine] = slab[mine]
    table[...] = jnp.zeros_like(table)
    arrived[pair(place(me))] = sent[pair(me)]

    lane = lax.broadcasted_iota(jnp.int32, (16, 128), 1)
    lane_f = lane.astype(jnp.float32)
    places = position[...]
    low_bits = (places + lax.shift_left(band[...], 11) + lax.shift_left(degree[...], 19)).astype(jnp.float32)
    allowed = jnp.zeros((16, 128), jnp.int32)
    for a in range(3):
        moves = jnp.concatenate([actions[a : a + 1, 128 * row : 128 * row + 128] for row in range(16)], axis=0)
        for n, offset in enumerate(OFFSETS):
            allowed = jnp.bitwise_or(allowed, jnp.where(moves == offset, 1 << n, 0))
    high_bits = allowed.astype(jnp.float32)
    volumes = volume[...]
    target = lax.shift_right_logical(places, 6)
    for h in range(2):
        here = (target == me) & ((lane >= 64) if h else (lane < 64))
        first = jnp.min(jnp.where(here, lane_f, 1000.0), axis=1, keepdims=True)
        last = jnp.max(jnp.where(here, lane_f, -1.0), axis=1, keepdims=True)
        for r, index in enumerate((first, last)):
            chosen = lane_f == index
            for n, value in enumerate((low_bits, high_bits, volumes)):
                total = jnp.sum(jnp.where(chosen, value, 0.0), axis=1, keepdims=True)
                params[n, r, 16 * h : 16 * h + 16, :] = jnp.broadcast_to(total, (16, 128))
    slot_row = jnp.zeros((1, 128), jnp.float32)
    for r in range(2):
        word = params[0, r].astype(jnp.int32)
        levels = jnp.bitwise_and(lax.shift_right_logical(word, 11), 255)
        live[r] = jnp.where(lane32 < levels, DISCOUNT, 0.0)
        slot = jnp.bitwise_and(word, 63).astype(jnp.float32)
        slot_row = slot_row + jnp.sum(jnp.where(lane32 == row32 + 32 * r, slot, 0.0), axis=0, keepdims=True)
    slots[...] = slot_row.astype(jnp.int32)

    for copy in shares:
        copy.wait_recv()
    total = slab_in[0]
    for q in range(1, GROUP):
        total = total + slab_in[q]
    for zz in range(Z):
        row_out[zz] = total[X * zz : X * zz + X].reshape(X, 1, 128)
    row_mid[z] = row_out[z]
    small_z = []
    for dz in range(1, Z):
        small_z.append(send(row_out.at[lax.rem(z + dz, Z)], row_mid.at[z], (mine, block(dz, 0))))
    send_grids(SECOND)

    eye = lax.broadcasted_iota(jnp.int32, (8, 128), 0) == lax.broadcasted_iota(jnp.int32, (8, 128), 1)
    system = total[32:40] / float(paths) + jnp.where(eye, RIDGE, 0.0)
    slot_of = {}
    for j in range(BASIS):
        inverse = 1.0 / jnp.sqrt(system[j : j + 1, j : j + 1])
        column = system[:, j : j + 1] * inverse
        across = system[j : j + 1, :] * inverse
        system = system - column * across
        slot_of[j, j] = len(slot_of)
        factor[slot_of[j, j]] = jnp.broadcast_to(inverse, (8, 128))
        for i in range(j + 1, BASIS):
            slot_of[i, j] = len(slot_of)
            factor[slot_of[i, j]] = jnp.broadcast_to(column[i : i + 1, :], (8, 128))

    for copy in small_z:
        copy.wait_recv()
    row_in[x] = row_mid[:, x]
    small_x = []
    for dx in range(1, X):
        small_x.append(send(row_mid.at[:, lax.rem(x + dx, X)], row_in.at[x], (mine, block(0, dx))))
    send_grids(THIRD)
    for copy in small_x:
        copy.wait_recv()
    for xx in range(X):
        share[pl.ds(16 * (xx % 2) + xx // 2, Z, stride=2), :] = row_in[xx].reshape(Z, 128)
    moments[mine] = share[...]
    gathers = []
    for d in range(1, GROUP):
        q = lax.rem(mine + d, GROUP)
        gathers.append(send(share, moments.at[mine], (q, me)))

    for copy in gathers:
        copy.wait_recv()
    lane8 = lax.broadcasted_iota(jnp.int32, (8, 128), 1)
    for tile in range(4):
        rows = slice(8 * tile, 8 * tile + 8)
        for r in range(2):
            word = params[0, r, rows, :].astype(jnp.int32)
            moves = params[1, r, rows, :].astype(jnp.int32)
            vol = params[2, r, rows, :]
            levels = jnp.bitwise_and(lax.shift_right_logical(word, 11), 255)
            highest = lax.shift_right_logical(word, 19)
            halfway, fitted = [], [None] * BASIS
            for i in range(BASIS):
                value = moments[8 * r + i, rows, :] / float(paths)
                for j in range(i):
                    value = value - factor[slot_of[i, j]] * halfway[j]
                halfway.append(value * factor[slot_of[i, i]])
            for i in reversed(range(BASIS)):
                value = halfway[i]
                for j in range(i + 1, BASIS):
                    value = value - factor[slot_of[j, i]] * fitted[j]
                fitted[i] = jnp.where(highest >= i, value * factor[slot_of[i, i]], 0.0)
            first = (16 * tile + r) * ROWS
            for n, offset in enumerate(OFFSETS):
                bit = jnp.bitwise_and(lax.shift_right_logical(moves, n), 1)
                to = lane8 + offset
                usable = (bit == 1) & (to >= 0) & (to < levels) & (lane8 < levels)
                for k in range(BASIS):
                    moved = pltpu.roll(fitted[k], (-offset) % LEVELS, 1)
                    table[pl.ds(first + 16 * n + k, 8, stride=2 * ROWS), :] = jnp.where(
                        usable, DISCOUNT * (moved - fitted[k]), 0.0
                    )
                table[pl.ds(first + 16 * n + BASIS, 8, stride=2 * ROWS), :] = jnp.where(
                    usable, -float(offset) * vol, 0.0
                )

    def best(c, carry):
        rows = table[pl.ds(pl.multiple_of(c * ROWS, 16), ROWS), :]
        value = jnp.zeros((128, 128), jnp.float32)
        for n in range(0, len(OFFSETS), 2):
            two = jnp.concatenate([rows[16 * n : 16 * n + 16], rows[16 * n + 16 : 16 * n + 32]], axis=1)
            two_high, two_low = split(two)
            right = jnp.concatenate([two_high, two_low, two_high], axis=0)
            result = jnp.dot(left[...], right, preferred_element_type=jnp.float32)
            value = jnp.maximum(value, jnp.maximum(result[:, :128], result[:, 128:]))
        gain[c] = value
        return carry

    lax.fori_loop(0, CON, best, 0, unroll=2)
    for copy in grids:
        copy.wait_recv()
    for copy in started:
        copy.wait_send()


SENDS = BLOCKS - 1 + Z - 1 + X - 1 + 2 * (GROUP - 1)


def finish_kernel(slots, arrived, gain, live, valued, ready, sem):
    for r in range(2):

        def one(row, carry):
            c = 2 * row + r
            kept = live[r, pl.ds(row, 1), :]
            ready[c] = (gain[c] + kept * arrived[c].astype(jnp.float32)).astype(jnp.bfloat16)
            pltpu.make_async_copy(ready.at[c], valued.at[slots[0, 32 * r + row]], sem).start()
            return carry

        lax.fori_loop(0, BLOCKS, one, 0)
    pltpu.make_async_copy(ready, valued, sem).wait()


def in_vmem(array):
    return pltpu.with_memory_space_constraint(array, pltpu.VMEM)


def kept_in_hbm(array):
    return pltpu.with_memory_space_constraint(array, pltpu.HBM)


def per_device(prices, terminal, band, position, actions, degree, volume):
    paths = prices.shape[1] * lax.axis_size("paths")
    con, width, levels = terminal.shape
    vmem = pl.BlockSpec(memory_space=pltpu.VMEM)
    anywhere = pl.BlockSpec(memory_space=pl.ANY)
    in_hbm = pl.BlockSpec(memory_space=pltpu.HBM)
    scalars = pl.BlockSpec(memory_space=pltpu.SMEM)
    grids = (con, width, levels)

    def table(array):
        return array.reshape(16, 128)

    dma = pltpu.SemaphoreType.DMA
    f32, bf16 = jnp.float32, jnp.bfloat16
    arrived, gain, live, slots = pl.pallas_call(
        functools.partial(exchange_kernel, paths),
        out_shape=(
            pltpu.VMEM(grids, bf16),
            pltpu.VMEM(grids, f32),
            pltpu.VMEM((2, 32, 128), f32),
            jax.ShapeDtypeStruct((1, 128), jnp.int32),
        ),
        in_specs=[in_hbm] * 7,
        out_specs=(vmem,) * 4,
        scratch_shapes=[
            pltpu.VMEM((1, width), f32),
            pltpu.VMEM(grids, bf16),
            pltpu.VMEM((1, 128), jnp.int32),
            pltpu.SMEM((1, 128), jnp.int32),
            pltpu.VMEM((16, 128), jnp.int32),
            pltpu.VMEM((16, 128), jnp.int32),
            pltpu.VMEM((16, 128), jnp.int32),
            pltpu.VMEM((3, 2048), jnp.int32),
            pltpu.VMEM((16, 128), f32),
            pltpu.VMEM(grids, bf16),
            pltpu.VMEM((512, 128), f32),
            pltpu.VMEM((GROUP, 40, 128), f32),
            pltpu.VMEM((GROUP, 40, 128), f32),
            pltpu.VMEM((Z, X, 1, 128), f32),
            pltpu.VMEM((Z, X, 1, 128), f32),
            pltpu.VMEM((X, Z, 1, 128), f32),
            pltpu.VMEM((32, 128), f32),
            pltpu.VMEM((GROUP, 32, 128), f32),
            pltpu.VMEM((36, 8, 128), f32),
            pltpu.VMEM((CON * ROWS, 128), f32),
            pltpu.VMEM((128, 48), bf16),
            pltpu.VMEM((3, 2, 32, 128), f32),
            dma((SENDS,)),
            dma((SENDS,)),
            dma((8,)),
        ],
        compiler_params=pltpu.CompilerParams(
            collective_id=0, has_side_effects=True, vmem_limit_bytes=24 * MIB
        ),
        name="exchange",
    )(
        *map(kept_in_hbm, (prices, terminal)),
        *map(kept_in_hbm, (*map(table, (position, band, degree)), actions.T, table(volume))),
    )

    return pl.pallas_call(
        finish_kernel,
        out_shape=jax.ShapeDtypeStruct(grids, bf16),
        in_specs=[scalars, vmem, vmem, vmem],
        out_specs=anywhere,
        scratch_shapes=[pltpu.VMEM(grids, bf16), dma],
        compiler_params=pltpu.CompilerParams(vmem_limit_bytes=16 * MIB),
        name="finish",
    )(slots, in_vmem(arrived), in_vmem(gain), in_vmem(live))


def solution(mesh):
    in_specs = (P(None, "paths"), P("contract", "paths", None), P(), P(), P(), P(), P())
    return jax.shard_map(
        per_device, mesh=mesh, in_specs=in_specs, out_specs=P("contract", "paths", None), check_vma=False
    )
```
